8 devices in a mesh: part: 1 (over z), col: 2 (over y), row: 4 (over x, core).
Axes of the slice: x: 2, y: 2, z: 1, core: 2. Of those that a mesh axis runs over, the one named last changes fastest.
Arguments:
- matrix: float32 [6144, 4, 192], P(('part', 'row'), 'col')
Outputs:
- output 1: float32 [6144, 4, 192], P(('part', 'row'), 'col')
- output 2: float32 [4, 192], P('part')
- output 3: float32 [4, 192, 192], P('part')
- output 4: float32 [6144, 768], P(('part', 'row'))
All inputs are finite; a program needn't handle non-finite values.
Results may differ from the reference program's by a relative error of at most 0.001.
Values sent between devices are 32-bit elements.
A program may use at most 1 GiB of HBM per device.

```python
import jax
import jax.numpy as jnp
from jax import lax

MAT_ROWS = 6144
BLOCK_COLS = 192
PROC_COLS = 2
PANELS_DEV = 2
NUM_PANELS = PANELS_DEV * PROC_COLS
NUM_COLS = NUM_PANELS * BLOCK_COLS
HIGHEST = lax.Precision.HIGHEST


def matmul(lhs_mat, rhs_mat):
    return jnp.dot(lhs_mat, rhs_mat, precision=HIGHEST, preferred_element_type=jnp.float32)


def entry_to_logical(entry_mat):
    return entry_mat.reshape(MAT_ROWS, PROC_COLS, PANELS_DEV, BLOCK_COLS).transpose(0, 2, 1, 3).reshape(MAT_ROWS, NUM_COLS)


def logical_to_entry(logical):
    return logical.reshape(MAT_ROWS, PANELS_DEV, PROC_COLS, BLOCK_COLS).transpose(0, 2, 1, 3).reshape(MAT_ROWS, NUM_PANELS, BLOCK_COLS)


def setup_inputs(seed: int = 0, part: int = 0) -> dict:
    part_key = jax.random.fold_in(jax.random.key(seed), part)
    key_base, key_block, key_sign = jax.random.split(part_key, 3)
    row_ids = jnp.arange(MAT_ROWS)[:, None]
    col_ids = jnp.arange(NUM_COLS)[None, :]
    base_noise = jax.random.normal(key_base, (MAT_ROWS, NUM_COLS), jnp.float32)
    block_noise = jax.random.normal(key_block, (MAT_ROWS, NUM_COLS), jnp.float32)
    diag_signs = (2 * jax.random.randint(key_sign, (1, NUM_COLS), 0, 2) - 1).astype(jnp.float32)
    in_block = (row_ids // BLOCK_COLS == col_ids // BLOCK_COLS) & (row_ids > col_ids)
    block_scale = 0.3 * (MAT_ROWS / BLOCK_COLS) ** 0.5
    diag_scale = 0.5 * MAT_ROWS ** 0.5
    logical = base_noise + jnp.where(in_block, block_scale * block_noise, 0.0)
    logical = logical + jnp.where(row_ids == col_ids, diag_scale * diag_signs, 0.0)
    return {"matrix": logical_to_entry(logical)}


def factor_panel(panel_in, diag0):
    row_ids = jnp.arange(MAT_ROWS)
    col_ids = jnp.arange(BLOCK_COLS)

    def column_step(col_step, carried):
        panel_work, refl_vecs, tau_vec = carried
        diag_row = diag0 + col_step
        column = lax.dynamic_index_in_dim(panel_work, col_step, axis=1, keepdims=False)
        x_col = jnp.where(row_ids >= diag_row, column, 0.0)
        alpha_val = lax.dynamic_index_in_dim(column, diag_row, keepdims=False)
        col_norm = jnp.sqrt(jnp.sum(x_col * x_col))
        beta_val = jnp.where(alpha_val >= 0, -col_norm, col_norm)
        tau_step = (beta_val - alpha_val) / beta_val
        at_diag = row_ids == diag_row
        reflector = jnp.where(row_ids > diag_row, x_col / (alpha_val - beta_val), jnp.where(at_diag, 1.0, 0.0))
        v_dots = jnp.where(col_ids > col_step, matmul(reflector, panel_work), 0.0)
        panel_work = panel_work - tau_step * reflector[:, None] * v_dots[None, :]
        new_col = jnp.where(row_ids < diag_row, column, jnp.where(at_diag, beta_val, reflector))
        is_col = col_ids == col_step
        panel_work = jnp.where(is_col[None, :], new_col[:, None], panel_work)
        refl_vecs = jnp.where(is_col[None, :], reflector[:, None], refl_vecs)
        tau_vec = jnp.where(is_col, tau_step, tau_vec)
        return panel_work, refl_vecs, tau_vec

    init_carry = (panel_in, jnp.zeros_like(panel_in), jnp.zeros((BLOCK_COLS,), jnp.float32))
    return lax.fori_loop(0, BLOCK_COLS, column_step, init_carry)


def build_tfac(refl_vecs, tau_vec):
    col_ids = jnp.arange(BLOCK_COLS)
    gram_mat = matmul(refl_vecs.T, refl_vecs)

    def t_step(col_step, t_fac):
        g_col = jnp.where(col_ids < col_step, lax.dynamic_index_in_dim(gram_mat, col_step, axis=1, keepdims=False), 0.0)
        tau_step = tau_vec[col_step]
        new_col = jnp.where(col_ids == col_step, tau_step, -tau_step * matmul(t_fac, g_col))
        return jnp.where(col_ids[None, :] == col_step, new_col[:, None], t_fac)

    return lax.fori_loop(0, BLOCK_COLS, t_step, jnp.zeros((BLOCK_COLS, BLOCK_COLS), jnp.float32))


def reference(matrix):
    col_pos = jnp.arange(NUM_COLS)

    def panel_step(work_mat, panel_idx):
        first_col = panel_idx * BLOCK_COLS
        panel_in = lax.dynamic_slice_in_dim(work_mat, first_col, BLOCK_COLS, axis=1)
        panel_out, refl_vecs, tau_vec = factor_panel(panel_in, first_col)
        t_fac = build_tfac(refl_vecs, tau_vec)
        work_mat = lax.dynamic_update_slice_in_dim(work_mat, panel_out, first_col, axis=1)
        proj_sum = matmul(t_fac.T, matmul(refl_vecs.T, work_mat))
        proj_sum = jnp.where(col_pos[None, :] >= first_col + BLOCK_COLS, proj_sum, 0.0)
        work_mat = work_mat - matmul(refl_vecs, proj_sum)
        return work_mat, (refl_vecs, t_fac)

    scanned = lax.scan(panel_step, entry_to_logical(matrix), jnp.arange(NUM_PANELS))
    work_mat = scanned[0]
    all_vecs = scanned[1][0]
    all_tfac = scanned[1][1]
    q_init = (jnp.arange(MAT_ROWS)[:, None] == col_pos[None, :]).astype(jnp.float32)

    def q_step(q_cur, panel_pair):
        refl_vecs = panel_pair[0]
        t_fac = panel_pair[1]
        inner_prod = matmul(t_fac, matmul(refl_vecs.T, q_cur))
        return q_cur - matmul(refl_vecs, inner_prod), None

    q_mat = lax.scan(q_step, q_init, (all_vecs, all_tfac), reverse=True)[0]
    tau_vals = jnp.diagonal(all_tfac, axis1=1, axis2=2)
    return logical_to_entry(work_mat), tau_vals, all_tfac, q_mat
```

```python
import functools
import jax
import jax.numpy as jnp
from jax import lax
from jax.experimental import pallas as pl
from jax.experimental.pallas import tpu as pltpu
from jax.sharding import PartitionSpec as P

HIGHEST = lax.Precision.HIGHEST
NB = 128
SB = 8
TILES = NB // SB
SLAB = 256
MESH = pl.DeviceIdType.MESH


def dot_high(lhs_mat, rhs_mat):
    return jnp.dot(lhs_mat, rhs_mat, precision=HIGHEST, preferred_element_type=jnp.float32)


def contract(einsum_form, lhs_mat, rhs_mat):
    return jnp.einsum(einsum_form, lhs_mat, rhs_mat, precision=HIGHEST, preferred_element_type=jnp.float32)


def dot_tn(lhs_mat, rhs_mat):
    return lax.dot_general(lhs_mat, rhs_mat, (((0,), (0,)), ((), ())), precision=HIGHEST, preferred_element_type=jnp.float32)


def dot_nt(lhs_mat, rhs_mat):
    return lax.dot_general(lhs_mat, rhs_mat, (((1,), (1,)), ((), ())), precision=HIGHEST, preferred_element_type=jnp.float32)


def factor_panel(panel_in, row_start, diag0, reduce_rows):
    rows_loc, panel_width = panel_in.shape
    global_rows = row_start + jnp.arange(rows_loc)
    col_ids = jnp.arange(panel_width)

    def column_step(col_step, carried):
        panel_work, refl_vecs, tau_vec = carried
        diag_row = diag0 + col_step
        column = lax.dynamic_index_in_dim(panel_work, col_step, axis=1, keepdims=False)
        x_col = jnp.where(global_rows >= diag_row, column, 0.0)
        local_row = diag_row - row_start
        holds_diag = (local_row >= 0) & (local_row < rows_loc)
        diag_row_vals = lax.dynamic_index_in_dim(panel_work, jnp.clip(local_row, 0, rows_loc - 1), axis=0, keepdims=False)
        diag_piece = jnp.where(holds_diag, diag_row_vals, 0.0)
        summed = reduce_rows(jnp.stack([dot_high(x_col, panel_work), diag_piece]))
        x_dots = summed[0]
        diag_vals = summed[1]
        alpha_val = diag_vals[col_step]
        col_norm = jnp.sqrt(x_dots[col_step])
        beta_val = jnp.where(alpha_val >= 0, -col_norm, col_norm)
        tau_step = (beta_val - alpha_val) / beta_val
        inv_scale = 1.0 / (alpha_val - beta_val)
        at_diag = global_rows == diag_row
        reflector = jnp.where(global_rows > diag_row, x_col * inv_scale, jnp.where(at_diag, 1.0, 0.0))
        v_dots = jnp.where(col_ids > col_step, inv_scale * (x_dots - alpha_val * diag_vals) + diag_vals, 0.0)
        panel_work = panel_work - tau_step * reflector[:, None] * v_dots[None, :]
        new_col = jnp.where(global_rows < diag_row, column, jnp.where(at_diag, beta_val, reflector))
        is_col = col_ids == col_step
        panel_work = jnp.where(is_col[None, :], new_col[:, None], panel_work)
        refl_vecs = jnp.where(is_col[None, :], reflector[:, None], refl_vecs)
        tau_vec = jnp.where(is_col, tau_step, tau_vec)
        return panel_work, refl_vecs, tau_vec

    init_carry = (panel_in, jnp.zeros_like(panel_in), jnp.zeros((panel_width,), jnp.float32))
    return lax.fori_loop(0, panel_width, column_step, init_carry)


def build_tfac(refl_vecs, tau_vec, reduce_rows):
    panel_width = tau_vec.shape[0]
    col_ids = jnp.arange(panel_width)
    gram_mat = reduce_rows(contract("rk,rl->kl", refl_vecs, refl_vecs))

    def t_step(col_step, t_fac):
        g_col = jnp.where(col_ids < col_step, lax.dynamic_index_in_dim(gram_mat, col_step, axis=1, keepdims=False), 0.0)
        tau_step = tau_vec[col_step]
        new_col = jnp.where(col_ids == col_step, tau_step, -tau_step * dot_high(t_fac, g_col))
        return jnp.where(col_ids[None, :] == col_step, new_col[:, None], t_fac)

    return lax.fori_loop(0, panel_width, t_step, jnp.zeros((panel_width, panel_width), jnp.float32))


def permute_sum(value, axis, size):
    stride = 1
    while stride < size:
        value = value + lax.ppermute(value, axis, [(i, i ^ stride) for i in range(size)])
        stride *= 2
    return value


def columnwise_program(a_loc, proc_cols, proc_rows):
    sum_rows = lambda value: permute_sum(value, "row", proc_rows)
    rows_loc, panels_loc, panel_width = a_loc.shape
    num_panels = panels_loc * proc_cols
    col_idx = lax.axis_index("col")
    row_start = lax.axis_index("row") * rows_loc
    global_rows = row_start + jnp.arange(rows_loc)
    panel_ids = jnp.arange(panels_loc) * proc_cols + col_idx

    def panel_step(panel_idx, carried):
        a_work, all_vecs, all_tfac = carried
        slot_idx = panel_idx // proc_cols
        is_owner = col_idx == panel_idx % proc_cols
        old_panel = lax.dynamic_index_in_dim(a_work, slot_idx, axis=1, keepdims=False)
        new_panel, refl_vecs, tau_vec = factor_panel(old_panel, row_start, panel_idx * panel_width, sum_rows)
        t_fac = build_tfac(refl_vecs, tau_vec, sum_rows)
        refl_vecs = permute_sum(jnp.where(is_owner, refl_vecs, 0.0), "col", proc_cols)
        t_fac = permute_sum(jnp.where(is_owner, t_fac, 0.0), "col", proc_cols)
        a_work = lax.dynamic_update_index_in_dim(a_work, jnp.where(is_owner, new_panel, old_panel), slot_idx, axis=1)
        proj_sum = sum_rows(contract("rk,rsj->ksj", refl_vecs, a_work))
        w_block = contract("kl,ksj->lsj", t_fac, proj_sum)
        w_block = jnp.where((panel_ids > panel_idx)[None, :, None], w_block, 0.0)
        a_work = a_work - contract("rl,lsj->rsj", refl_vecs, w_block)
        all_vecs = lax.dynamic_update_index_in_dim(all_vecs, refl_vecs, panel_idx, axis=0)
        all_tfac = lax.dynamic_update_index_in_dim(all_tfac, t_fac, panel_idx, axis=0)
        return a_work, all_vecs, all_tfac

    init_carry = (a_loc, jnp.zeros((num_panels, rows_loc, panel_width), jnp.float32), jnp.zeros((num_panels, panel_width, panel_width), jnp.float32))
    a_work, all_vecs, all_tfac = lax.fori_loop(0, num_panels, panel_step, init_carry)
    logical_cols = panel_ids[:, None] * panel_width + jnp.arange(panel_width)[None, :]
    q_init = (global_rows[:, None, None] == logical_cols[None, :, :]).astype(jnp.float32)

    def q_step(back_step, q_local):
        panel_idx = num_panels - 1 - back_step
        refl_vecs = lax.dynamic_index_in_dim(all_vecs, panel_idx, keepdims=False)
        t_fac = lax.dynamic_index_in_dim(all_tfac, panel_idx, keepdims=False)
        proj_sum = sum_rows(contract("rk,rsj->ksj", refl_vecs, q_local))
        w_block = contract("kl,lsj->ksj", t_fac, proj_sum)
        return q_local - contract("rk,ksj->rsj", refl_vecs, w_block)

    q_local = lax.fori_loop(0, num_panels, q_step, q_init)
    placed = jnp.where((jnp.arange(proc_cols) == col_idx)[None, None, :, None], q_local[:, :, None, :], 0.0)
    q_rows = permute_sum(placed, "col", proc_cols).reshape(rows_loc, num_panels * panel_width)
    tau_vals = jnp.diagonal(all_tfac, axis1=1, axis2=2)
    return a_work, tau_vals, all_tfac, q_rows


def _iota(dim):
    return lax.broadcasted_iota(jnp.int32, (SB, NB), dim)


def _lane(tile, lane_id):
    return jnp.broadcast_to(tile[:, lane_id : lane_id + 1], (SB, NB))


def _sub(tile, sub_id):
    return jnp.broadcast_to(tile[sub_id : sub_id + 1, :], (SB, NB))


def _set_identity(ref):
    for i in range(TILES):
        ref[SB * i : SB * (i + 1), :] = (_iota(1) == _iota(0) + SB * i).astype(jnp.float32)


def _tile(ref, i):
    return ref[SB * i : SB * (i + 1), :]


def chol_block(d_ref, e_ref):
    sub = _iota(0)
    lane = _iota(1)
    _set_identity(e_ref)
    for b in range(TILES):
        row_d = _tile(d_ref, b)
        row_e = _tile(e_ref, b)
        diag_cols = [_lane(row_d, SB * b + j) for j in range(SB)]
        scale = jnp.zeros((SB, NB), jnp.float32)
        inv, coef, rows_d, rows_e = [], [], [], []
        for j in range(SB):
            pivot = _sub(diag_cols[j], j)
            inv_j = 1.0 / pivot
            scale = jnp.where(sub == j, lax.rsqrt(pivot), scale)
            mult = jnp.where(sub > j, diag_cols[j] * inv_j, 0.0)
            coef_j = {}
            for jj in range(j + 1, SB):
                coef_j[jj] = _sub(diag_cols[jj], j)
                diag_cols[jj] = diag_cols[jj] - mult * coef_j[jj]
            rd = _sub(row_d, j)
            re = _sub(row_e, j)
            row_d = row_d - mult * rd
            row_e = row_e - mult * re
            inv.append(inv_j)
            coef.append(coef_j)
            rows_d.append(rd)
            rows_e.append(re)
        d_ref[SB * b : SB * (b + 1), :] = jnp.where(lane >= sub + SB * b, row_d * scale, 0.0)
        e_ref[SB * b : SB * (b + 1), :] = row_e * scale
        for i in range(b + 1, TILES):
            tile_d = _tile(d_ref, i)
            tile_e = _tile(e_ref, i)
            cols = [_lane(tile_d, SB * b + j) for j in range(SB)]
            for j in range(SB):
                mult = cols[j] * inv[j]
                for jj in range(j + 1, SB):
                    cols[jj] = cols[jj] - mult * coef[j][jj]
                tile_d = tile_d - mult * rows_d[j]
                tile_e = tile_e - mult * rows_e[j]
            d_ref[SB * i : SB * (i + 1), :] = tile_d
            e_ref[SB * i : SB * (i + 1), :] = tile_e


def lu_block(w_ref, r_ref, p_ref, e_ref, pi_ref, s_ref):
    sub = _iota(0)
    lane = _iota(1)
    _set_identity(e_ref)
    _set_identity(pi_ref)
    for b in range(TILES):
        row_w = _tile(w_ref, b)
        row_e = _tile(e_ref, b)
        row_r = _tile(r_ref, b)
        later = lane >= SB * (b + 1)
        diag_cols = [_lane(row_w, SB * b + j) for j in range(SB)]
        norm_cols = [_lane(row_r, SB * b + j) for j in range(SB)]
        signs = jnp.zeros((SB, NB), jnp.float32)
        p_tile = jnp.zeros((SB, NB), jnp.float32)
        l_tile = row_w
        inv, coef, rows_p, rows_e = [], [], [], []
        for j in range(SB):
            alpha = _sub(diag_cols[j], j)
            norm = _sub(norm_cols[j], j)
            sign = jnp.where(alpha >= 0, -1.0, 1.0)
            inv_j = 1.0 / (alpha - sign * norm)
            mult = jnp.where(sub > j, diag_cols[j] * inv_j, 0.0)
            coef_j = {}
            for jj in range(j + 1, SB):
                coef_j[jj] = _sub(diag_cols[jj], j) - sign * _sub(norm_cols[jj], j)
                diag_cols[jj] = diag_cols[jj] - mult * coef_j[jj]
            rp = _sub(row_w, j) - sign * _sub(row_r, j)
            re = _sub(row_e, j)
            row_w = row_w - mult * rp
            row_e = row_e - mult * re
            signs = jnp.where(sub == j, sign, signs)
            p_tile = jnp.where(sub == j, rp, p_tile)
            l_tile = jnp.where(lane == SB * b + j, mult, l_tile)
            inv.append(inv_j)
            coef.append(coef_j)
            rows_p.append(jnp.where(later, rp, 0.0))
            rows_e.append(re)
        s_ref[SB * b : SB * (b + 1), :] = signs
        e_ref[SB * b : SB * (b + 1), :] = row_e
        p_ref[SB * b : SB * (b + 1), :] = jnp.where(lane >= sub + SB * b, p_tile, 0.0)
        l_tile = jnp.where(lane == sub + SB * b, 1.0, l_tile)
        w_ref[SB * b : SB * (b + 1), :] = jnp.where(lane <= sub + SB * b, l_tile, 0.0)
        for i in range(b + 1, TILES):
            tile_w = _tile(w_ref, i)
            tile_e = _tile(e_ref, i)
            cols = [_lane(tile_w, SB * b + j) for j in range(SB)]
            for j in range(SB):
                mult = cols[j] * inv[j]
                for jj in range(j + 1, SB):
                    cols[jj] = cols[jj] - mult * coef[j][jj]
                tile_w = jnp.where(lane == SB * b + j, mult, tile_w - mult * rows_p[j])
                tile_e = tile_e - mult * rows_e[j]
            w_ref[SB * i : SB * (i + 1), :] = tile_w
            e_ref[SB * i : SB * (i + 1), :] = tile_e
        for i in range(b + 1):
            tile_pi = _tile(pi_ref, i)
            cols = [_lane(tile_pi, SB * b + j) for j in range(SB)]
            for j in range(SB):
                mult = cols[j] * inv[j]
                for jj in range(j + 1, SB):
                    cols[jj] = cols[jj] - mult * coef[j][jj]
                tile_pi = jnp.where(lane == SB * b + j, mult, tile_pi - mult * rows_p[j])
            pi_ref[SB * i : SB * (i + 1), :] = tile_pi


def window_starts(n, panels):
    width = n // panels
    return [min(width * g // NB * NB, n - 2 * NB) for g in range(panels)]


def slab_starts(n):
    starts, at = [], 0
    for top in range(0, n, SLAB):
        starts.append(at)
        at += n - top
    return starts, at


def gram_view(g_ref, n, lo, hi, first, last):
    starts, _ = slab_starts(n)
    slab = lo // SLAB
    base = starts[slab] - SLAB * slab
    return g_ref[lo - SLAB * slab : hi - SLAB * slab, base + first : base + last]


def factor_kernel(n, g_ref, at_ref, ft_ref, xt_ref, pit_ref, t_ref, tau_ref, flag_ref, a_ref, l_ref, p_ref, rh_ref, li_ref, pi_ref, d_ref, e_ref, w_ref, lie_ref, pd_ref, pie_ref, s_ref):
    blocks = n // NB
    for ref in (xt_ref, pi_ref, l_ref, p_ref, rh_ref, li_ref):
        ref[...] = jnp.zeros_like(ref)
    a_ref[...] = at_ref[...].T

    def block_step(g, carry):
        for i in range(blocks):
            lo = NB * i
            hi = lo + NB

            @pl.when(g == i)
            def _():
                d_new = gram_view(g_ref, n, lo, hi, lo, hi)
                w_new = a_ref[lo:hi, lo:hi]
                if i:
                    r_col = rh_ref[0:lo, lo:hi]
                    d_new = d_new - dot_tn(r_col, r_col)
                    w_new = w_new - dot_high(l_ref[lo:hi, 0:lo], p_ref[0:lo, lo:hi])
                d_ref[...] = d_new
                w_ref[...] = w_new

        chol_block(d_ref, e_ref)
        lu_block(w_ref, d_ref, pd_ref, lie_ref, pie_ref, s_ref)

        for i in range(blocks):
            lo = NB * i
            hi = lo + NB

            @pl.when(g == i)
            def _():
                signs = s_ref[...]
                r_gg = signs * d_ref[...]
                xt_gg = signs * e_ref[...]
                l_gg = w_ref[...]
                li_gg = lie_ref[...]
                p_gg = pd_ref[...]
                pi_gg = pie_ref[...]
                rh_ref[lo:hi, lo:hi] = r_gg
                xt_ref[lo:hi, lo:hi] = xt_gg
                l_ref[lo:hi, lo:hi] = l_gg
                li_ref[lo:hi, lo:hi] = li_gg
                p_ref[lo:hi, lo:hi] = p_gg
                pi_ref[lo:hi, lo:hi] = pi_gg
                if hi < n:
                    g_row = gram_view(g_ref, n, lo, hi, hi, n)
                    w_row = a_ref[lo:hi, hi:n]
                    w_col = a_ref[hi:n, lo:hi]
                    if i:
                        g_row = g_row - dot_tn(rh_ref[0:lo, lo:hi], rh_ref[0:lo, hi:n])
                        w_row = w_row - dot_high(l_ref[lo:hi, 0:lo], p_ref[0:lo, hi:n])
                        w_col = w_col - dot_high(l_ref[hi:n, 0:lo], p_ref[0:lo, lo:hi])
                    r_row = dot_high(xt_gg, g_row)
                    rh_ref[lo:hi, hi:n] = r_row
                    p_ref[lo:hi, hi:n] = dot_high(li_gg, w_row - r_row)
                    l_ref[hi:n, lo:hi] = dot_high(w_col, pi_gg)
                if i:
                    xt_ref[lo:hi, 0:lo] = -dot_high(xt_gg, dot_tn(rh_ref[0:lo, lo:hi], xt_ref[0:lo, 0:lo]))
                    pi_ref[0:lo, lo:hi] = -dot_high(pi_ref[0:lo, 0:lo], dot_high(p_ref[0:lo, lo:hi], pi_gg))
                    prev = lo - NB
                    li_ref[lo:hi, prev:lo] = -dot_high(li_gg, dot_high(l_ref[lo:hi, prev:lo], li_ref[prev:lo, prev:lo]))

        return carry

    lax.fori_loop(0, blocks, block_step, 0)
    rows = lax.broadcasted_iota(jnp.int32, (n, n), 0)
    cols = lax.broadcasted_iota(jnp.int32, (n, n), 1)
    ft_ref[...] = jnp.where(rows <= cols, rh_ref[...], l_ref[...]).T
    pit_ref[...] = pi_ref[...].T
    windows = t_ref.shape[0]
    for w, start in enumerate(window_starts(n, windows)):
        win = slice(start, start + 2 * NB)
        t_win = -dot_nt(dot_nt(p_ref[win, win], xt_ref[win, win]), li_ref[win, win])
        width = t_ref.shape[1]
        off = width * w - start
        if off:
            t_win = pltpu.roll(t_win[off : off + width], 2 * NB - off, 1)
        t_fac = t_win[0:width, 0:width]
        t_ref[w] = t_fac
        t_diag = lax.broadcasted_iota(jnp.int32, (width, width), 0) == lax.broadcasted_iota(jnp.int32, (width, width), 1)
        tau_ref[w : w + 1, :] = jnp.sum(jnp.where(t_diag, t_fac, 0.0), axis=0, keepdims=True)
    total = jnp.zeros((1, 1), jnp.float32)
    on_diag = lax.broadcasted_iota(jnp.int32, (NB, NB), 0) == lax.broadcasted_iota(jnp.int32, (NB, NB), 1)
    for lo in range(0, n, NB):
        hi = lo + NB
        diag = jnp.sum(jnp.where(on_diag, gram_view(g_ref, n, lo, hi, lo, hi), 0.0), axis=0, keepdims=True)
        block = xt_ref[lo:n, lo:hi]
        total = total + jnp.sum(diag * jnp.sum(block * block, axis=0, keepdims=True), axis=1, keepdims=True)
    flag_ref[...] = jnp.broadcast_to(total, flag_ref.shape)


def factor_call(gram, top_t, panels):
    n = top_t.shape[0]
    square = jax.ShapeDtypeStruct((n, n), jnp.float32)
    vmem = pl.BlockSpec(memory_space=pltpu.VMEM)
    return pl.pallas_call(
        functools.partial(factor_kernel, n),
        out_shape=(
            square,
            square,
            square,
            jax.ShapeDtypeStruct((panels, n // panels, n // panels), jnp.float32),
            jax.ShapeDtypeStruct((panels, n // panels), jnp.float32),
            jax.ShapeDtypeStruct((SB, NB), jnp.float32),
        ),
        in_specs=[vmem, vmem],
        out_specs=(vmem,) * 6,
        scratch_shapes=[pltpu.VMEM((n, n), jnp.float32)] * 6 + [pltpu.VMEM((NB, NB), jnp.float32)] * 7,
        compiler_params=pltpu.CompilerParams(vmem_limit_bytes=60 * 1024 * 1024),
        cost_estimate=pl.CostEstimate(flops=20_000_000_000, bytes_accessed=20_000_000, transcendentals=0),
    )(gram, top_t)


def gram_kernel(at_ref, g_ref, top_ref, got_ref, got_s, top_s, full_s, part_s, red_s, r0_s, r1_s, r2_s, r3_s, half_send, half_recv, top_recv, top_xs, top_cs, top_ys, red_send, red_recv):
    panels_loc, width, rows_loc = at_ref.shape
    n = full_s.shape[0]
    half = rows_loc // 2
    chunk = full_s.shape[1]
    chunks = half // chunk
    col = lax.axis_index("col")
    row = lax.axis_index("row")
    core = row % 2
    to_y = {"col": 1 - col}
    to_core = {"row": row + 1 - 2 * core}
    to_x = {"row": (row + 2) % 4}
    barrier = pltpu.get_barrier_semaphore()
    for dev in (to_y, to_core, to_x):
        pl.semaphore_signal(barrier, inc=1, device_id=dev, device_id_type=MESH)
    pl.semaphore_wait(barrier, 3)

    def remote(src, dst, send, recv, dev):
        return pltpu.make_async_remote_copy(src_ref=src, dst_ref=dst, send_sem=send, recv_sem=recv, device_id=dev, device_id_type=MESH)

    halves = []
    for k in range(chunks):
        lanes = pl.ds(pl.multiple_of(half * (1 - col) + chunk * k, NB), chunk)
        copy = remote(at_ref.at[:, :, lanes], got_s.at[:, :, chunk * k : chunk * (k + 1)], half_send.at[k], half_recv.at[k], to_y)
        copy.start()
        halves.append(copy)

    top_chunk = n // chunks

    def top_copies(src, which, send, dev):
        pieces = [slice(top_chunk * k, top_chunk * (k + 1)) for k in range(chunks)]
        return [remote(src.at[:, :, p], top_s.at[which, :, :, p], send.at[k], top_recv.at[which, k], dev) for k, p in enumerate(pieces)]

    own_top = at_ref.at[:, :, 0:n]
    is_first = (row == 0) & (col == 0)
    is_second = (row == 0) & (col == 1)

    @pl.when(row == 0)
    def _():
        for to_one, to_two in zip(top_copies(own_top, col, top_xs.at[0], to_x), top_copies(own_top, col, top_cs.at[0], to_core)):
            to_one.start()
            to_two.start()

    @pl.when(is_first)
    def _():
        for copy in top_copies(own_top, 0, top_ys, to_y):
            copy.start()

    starts, _ = slab_starts(n)
    for k in range(chunks):
        halves[k].wait_recv()

        @pl.when(is_first)
        def _(k=k):
            top_copies(got_s, 1, top_xs.at[1], to_x)[k].start()
            top_copies(got_s, 1, top_cs.at[1], to_core)[k].start()

        mine = pl.ds(pl.multiple_of(half * col + chunk * k, NB), chunk)
        for s in range(panels_loc):
            full_s[pl.ds(pl.multiple_of(width * (2 * s + col), SB), width), :] = at_ref[s, :, mine]
            full_s[pl.ds(pl.multiple_of(width * (2 * s + 1 - col), SB), width), :] = got_s[s, :, chunk * k : chunk * (k + 1)]
        for i, at in enumerate(starts):
            lo = SLAB * i
            add = dot_nt(full_s[lo : lo + SLAB, :], full_s[lo:n, :])
            if k:
                add = add + part_s[:, at : at + n - lo]
            part_s[:, at : at + n - lo] = add

    per_core = SLAB // 2
    quarter = per_core // 2
    mine = pl.ds(pl.multiple_of(per_core * core, SB), per_core)
    other = pl.ds(pl.multiple_of(per_core * (1 - core), SB), per_core)
    pair = remote(part_s.at[other, :], r0_s, red_send.at[0], red_recv.at[0], to_core)
    pair.start()
    pair.wait_recv()
    red_s[0] = part_s[mine, :] + r0_s[...]
    first = [
        remote(red_s.at[0, 0:quarter, :], r1_s.at[0], red_send.at[1], red_recv.at[1], to_x),
        remote(red_s.at[0, quarter:per_core, :], r1_s.at[1], red_send.at[2], red_recv.at[2], to_y),
    ]
    for copy in first:
        copy.start()

    @pl.when(is_second)
    def _():
        came = top_copies(own_top, 0, top_ys, to_y)
        for k, copy in enumerate(came):
            copy.wait_recv()
            top_copies(top_s.at[0], 0, top_xs.at[1], to_x)[k].start()
            top_copies(top_s.at[0], 0, top_cs.at[1], to_core)[k].start()

    for k, copy in enumerate(first):
        copy.wait_recv()
        red_s[1, quarter * k : quarter * (k + 1), :] = red_s[0, quarter * k : quarter * (k + 1), :] + r1_s[k]
    second = [
        remote(red_s.at[1, 0:quarter, :], r2_s.at[0], red_send.at[3], red_recv.at[3], to_y),
        remote(red_s.at[1, quarter:per_core, :], r2_s.at[1], red_send.at[4], red_recv.at[4], to_x),
    ]
    for copy in second:
        copy.start()

    for k, copy in enumerate(second):
        copy.wait_recv()
        red_s[2, quarter * k : quarter * (k + 1), :] = red_s[1, quarter * k : quarter * (k + 1), :] + r2_s[k]
    last = remote(red_s.at[2], r3_s, red_send.at[5], red_recv.at[5], to_core)
    last.start()
    g_ref[mine, :] = red_s[2]

    @pl.when(row == 2)
    def _():
        for step in range(2):
            which = col if step == 0 else 1 - col
            came = top_copies(own_top, which, top_xs.at[step], to_x)
            sent = top_copies(top_s.at[which], which, top_cs.at[step], to_core)
            for k in range(chunks):
                came[k].wait_recv()
                sent[k].start()

    last.wait_recv()
    g_ref[other, :] = r3_s[...]

    @pl.when(core == 1)
    def _():
        for step in range(2):
            for copy in top_copies(own_top, col if step == 0 else 1 - col, top_cs.at[step], to_core):
                copy.wait_recv()

    got_ref[...] = got_s[...]
    for s in range(panels_loc):
        for k in range(2):
            top_ref[2 * s + k] = top_s[k, s]

    @pl.when(row == 0)
    def _():
        for s in range(panels_loc):
            top_ref[2 * s + col] = at_ref[s, :, 0:n]

    @pl.when((row == 0) & (col == 0))
    def _():
        for s in range(panels_loc):
            top_ref[2 * s + 1] = got_s[s]

    for copy in halves + [pair] + first + second + [last]:
        copy.wait_send()

    @pl.when(is_first)
    def _():
        for copy in top_copies(own_top, 0, top_ys, to_y):
            copy.wait_send()

    @pl.when(row == 0)
    def _():
        for step in range(2):
            for copy in top_copies(own_top, col, top_xs.at[step], to_x):
                copy.wait_send()

    @pl.when(core == 0)
    def _():
        for step in range(2):
            for copy in top_copies(own_top, col, top_cs.at[step], to_core):
                copy.wait_send()


def gram_call(a_t, n):
    panels_loc, width, rows_loc = a_t.shape
    half = rows_loc // 2
    _, packed = slab_starts(n)
    vmem = pl.BlockSpec(memory_space=pltpu.VMEM)
    per_core = SLAB // 2
    f32 = lambda *shape: pltpu.VMEM(shape, jnp.float32)
    dma = pltpu.SemaphoreType.DMA
    chunks = 3
    return pl.pallas_call(
        gram_kernel,
        out_shape=(
            jax.ShapeDtypeStruct((SLAB, packed), jnp.float32),
            jax.ShapeDtypeStruct((2 * panels_loc, width, n), jnp.float32),
            jax.ShapeDtypeStruct((panels_loc, width, half), jnp.float32),
        ),
        in_specs=[vmem],
        out_specs=(vmem,) * 3,
        scratch_shapes=[
            f32(panels_loc, width, half),
            f32(2, panels_loc, width, n),
            f32(n, half // chunks),
            f32(SLAB, packed),
            f32(3, per_core, packed),
            f32(per_core, packed),
            f32(2, per_core // 2, packed),
            f32(2, per_core // 2, packed),
            f32(per_core, packed),
            dma((chunks,)),
            dma((chunks,)),
            dma((2, chunks)),
            dma((2, chunks)),
            dma((2, chunks)),
            dma((chunks,)),
            dma((6,)),
            dma((6,)),
        ],
        compiler_params=pltpu.CompilerParams(vmem_limit_bytes=60 * 1024 * 1024, collective_id=0, has_side_effects=True),
        cost_estimate=pl.CostEstimate(flops=10_000_000_000, bytes_accessed=10_000_000, transcendentals=0),
    )(a_t)


def apply_kernel(at_ref, got_ref, far_ref, xt_ref, pit_ref, ft_ref, q_ref, v_ref, full_s, own_s):
    panels_loc, width, chunk = at_ref.shape
    n = xt_ref.shape[0]
    step = pl.program_id(0)
    col = lax.axis_index("col")
    row = lax.axis_index("row")
    steps_half = pl.num_programs(0) // 2
    near = (step // steps_half) == col

    for s in range(panels_loc):
        full_s[pl.ds(pl.multiple_of(width * (2 * s + col), SB), width), :] = at_ref[s]
        full_s[pl.ds(pl.multiple_of(width * (2 * s + 1 - col), SB), width), :] = jnp.where(near, got_ref[s], far_ref[s])
    for lo in range(0, n, SLAB):
        hi = lo + SLAB
        q_ref[:, lo:hi] = lax.dot_general(full_s[0:hi, :], xt_ref[lo:hi, 0:hi], (((0,), (1,)), ((), ())), precision=HIGHEST, preferred_element_type=jnp.float32)
    is_top = (row == 0) & (step < n // chunk)

    @pl.when(jnp.logical_not(is_top))
    def _():
        for s in range(panels_loc):
            depth = width * 2 * (s + 1)
            rows = pl.ds(pl.multiple_of(width * (2 * s + col), SB), width)
            v_ref[s] = dot_high(pit_ref[rows, 0:depth], full_s[0:depth, :])

    @pl.when(is_top)
    def _():
        lanes = pl.ds(pl.multiple_of(jnp.minimum(step, n // chunk - 1) * chunk, NB), chunk)
        for s in range(panels_loc):
            rows = pl.ds(pl.multiple_of(width * (2 * s + col), SB), width)
            v_ref[s] = ft_ref[rows, lanes]


def apply_call(a_t, got, far, x_t, pi_t, f_t):
    panels_loc, width, rows_loc = a_t.shape
    n = x_t.shape[0]
    chunk = 256
    steps = rows_loc // chunk
    half_steps = steps // 2
    part = lambda index: pl.BlockSpec((panels_loc, width, chunk), index)
    whole = pl.BlockSpec(memory_space=pltpu.VMEM)
    return pl.pallas_call(
        apply_kernel,
        grid=(steps,),
        out_shape=(jax.ShapeDtypeStruct((rows_loc, n), jnp.float32), jax.ShapeDtypeStruct((panels_loc, width, rows_loc), jnp.float32)),
        in_specs=[part(lambda i: (0, 0, i)), part(lambda i: (0, 0, i % half_steps)), part(lambda i: (0, 0, i % half_steps)), whole, whole, whole],
        out_specs=(pl.BlockSpec((chunk, n), lambda i: (i, 0)), part(lambda i: (0, 0, i))),
        scratch_shapes=[pltpu.VMEM((n, chunk), jnp.float32), pltpu.VMEM((SB, NB), jnp.float32)],
        compiler_params=pltpu.CompilerParams(vmem_limit_bytes=60 * 1024 * 1024),
        cost_estimate=pl.CostEstimate(flops=5_000_000_000, bytes_accessed=20_000_000, transcendentals=0),
    )(a_t, got, far, x_t, pi_t, f_t)


def solution(mesh):
    proc_cols = mesh.shape["col"]

    def local_program(a_loc):
        rows_loc, panels_loc, panel_width = a_loc.shape
        num_panels = panels_loc * proc_cols
        n = num_panels * panel_width
        col_idx = lax.axis_index("col")
        half = rows_loc // proc_cols
        a_t = a_loc.transpose(1, 2, 0)
        gram, top_t, got = gram_call(a_t, n)
        own_half = lax.dynamic_slice_in_dim(a_t, col_idx * half, half, axis=2)
        own_half, gram, top_t, got = lax.optimization_barrier((own_half, gram, top_t, got))
        far = lax.ppermute(own_half, "col", [(0, 1), (1, 0)])
        f_t, x_t, pi_t, t_facs, taus, flag = factor_call(gram, top_t.reshape(n, n), num_panels)
        well = flag[0, 0] < 2.0 * n

        def gram_path(_):
            q_rows, vecs = apply_call(a_t, got, far, x_t, pi_t, f_t)
            return vecs.transpose(2, 0, 1), taus, t_facs, q_rows

        return lax.cond(well, gram_path, lambda _: columnwise_program(a_loc, proc_cols, mesh.shape["row"]), 0)

    spec_rows = P(("part", "row"), "col", None)
    out_specs = (spec_rows, P("part", None), P("part", None, None), P(("part", "row"), None))
    return jax.shard_map(local_program, mesh=mesh, in_specs=(spec_rows,), out_specs=out_specs, check_vma=False)
```

```python
import functools
import jax
import jax.numpy as jnp
from jax import lax
from jax.experimental import pallas as pl
from jax.experimental.pallas import tpu as pltpu
from jax.sharding import PartitionSpec as P

HIGHEST = lax.Precision.HIGHEST
NB = 128
SB = 8
TILES = NB // SB
SLAB = 256
MESH = pl.DeviceIdType.MESH


def dot_high(lhs_mat, rhs_mat):
    return jnp.dot(lhs_mat, rhs_mat, precision=HIGHEST, preferred_element_type=jnp.float32)


def dot_tn(lhs_mat, rhs_mat):
    return lax.dot_general(lhs_mat, rhs_mat, (((0,), (0,)), ((), ())), precision=HIGHEST, preferred_element_type=jnp.float32)


def dot_nt(lhs_mat, rhs_mat):
    return lax.dot_general(lhs_mat, rhs_mat, (((1,), (1,)), ((), ())), precision=HIGHEST, preferred_element_type=jnp.float32)


def permute_sum(value, axis, size):
    stride = 1
    while stride < size:
        value = value + lax.ppermute(value, axis, [(i, i ^ stride) for i in range(size)])
        stride *= 2
    return value


def columnwise_program(a_t, proc_cols, proc_rows):
    panels_loc, width, rows_loc = a_t.shape
    num_panels = panels_loc * proc_cols
    cols_loc = panels_loc * width
    col_idx = lax.axis_index("col")
    row_start = lax.axis_index("row") * rows_loc
    rows = row_start + lax.broadcasted_iota(jnp.int32, (1, rows_loc), 1)
    local_cols = lax.broadcasted_iota(jnp.int32, (cols_loc, 1), 0)
    col_ids = (local_cols // width * proc_cols + col_idx) * width + local_cols % width
    in_panel = lax.broadcasted_iota(jnp.int32, (width, 1), 0)

    def column_step(k, carried):
        work, vecs, taus, t_facs = carried
        panel = k // width
        inner = k % width
        own = panel % proc_cols == col_idx
        column = lax.dynamic_slice_in_dim(work, panel // proc_cols * width + inner, 1, axis=0)
        column = permute_sum(jnp.where(own, column, 0.0), "col", proc_cols)
        x_col = jnp.where(rows >= k, column, 0.0)
        at_diag = rows == k
        panel_vecs = lax.dynamic_slice_in_dim(vecs, panel * width, width, axis=0)
        stacked = jnp.concatenate([work, x_col, panel_vecs], axis=0)
        dots = permute_sum(jnp.sum(stacked * x_col, axis=1, keepdims=True), "row", proc_rows)
        diag = permute_sum(jnp.sum(jnp.where(at_diag, stacked, 0.0), axis=1, keepdims=True), "row", proc_rows)
        alpha = diag[cols_loc, 0]
        norm = jnp.sqrt(dots[cols_loc, 0])
        beta = jnp.where(alpha >= 0, -norm, norm)
        tau = (beta - alpha) / beta
        inv_scale = 1.0 / (alpha - beta)
        reflector = jnp.where(rows > k, x_col * inv_scale, jnp.where(at_diag, 1.0, 0.0))
        v_dots = inv_scale * (dots - alpha * diag) + diag
        work = work - jnp.where(col_ids > k, tau * v_dots[:cols_loc], 0.0) * reflector
        work = jnp.where(col_ids == k, jnp.where(rows < k, column, jnp.where(at_diag, beta, reflector)), work)
        t_fac = lax.dynamic_index_in_dim(t_facs, panel, keepdims=False)
        g_col = jnp.where(in_panel < inner, v_dots[cols_loc + 1 :], 0.0)
        t_col = jnp.where(in_panel == inner, tau, -tau * jnp.sum(t_fac * g_col.reshape(1, width), axis=1, keepdims=True))
        t_fac = jnp.where(in_panel.reshape(1, width) == inner, t_col, t_fac)
        t_facs = lax.dynamic_update_index_in_dim(t_facs, t_fac, panel, axis=0)
        return work, lax.dynamic_update_slice_in_dim(vecs, reflector, k, axis=0), lax.dynamic_update_index_in_dim(taus, tau, k, axis=0), t_facs

    n = num_panels * width
    zeros = lambda *shape: jnp.zeros(shape, jnp.float32)
    work, vecs, taus, t_facs = lax.fori_loop(0, n, column_step, (a_t.reshape(cols_loc, rows_loc), zeros(n, rows_loc), zeros(n), zeros(num_panels, width, width)))

    def q_step(step, q_cols):
        k = n - 1 - step
        reflector = lax.dynamic_slice_in_dim(vecs, k, 1, axis=0)
        dots = permute_sum(jnp.sum(q_cols * reflector, axis=1, keepdims=True), "row", proc_rows)
        return q_cols - taus[k] * dots * reflector

    q_cols = lax.fori_loop(0, n, q_step, (col_ids == rows).astype(jnp.float32)).reshape(panels_loc, width, rows_loc)
    placed = jnp.stack([jnp.where(col_idx == c, q_cols, 0.0) for c in range(proc_cols)], axis=1)
    q_rows = permute_sum(placed, "col", proc_cols).reshape(n, rows_loc).T
    return work.reshape(panels_loc, width, rows_loc).transpose(2, 0, 1), taus.reshape(num_panels, width), t_facs, q_rows


def _iota(dim):
    return lax.broadcasted_iota(jnp.int32, (SB, NB), dim)


def _lane(tile, lane_id):
    return jnp.broadcast_to(tile[:, lane_id : lane_id + 1], (SB, NB))


def _sub(tile, sub_id):
    return jnp.broadcast_to(tile[sub_id : sub_id + 1, :], (SB, NB))


def _set_identity(ref):
    for i in range(TILES):
        ref[SB * i : SB * (i + 1), :] = (_iota(1) == _iota(0) + SB * i).astype(jnp.float32)


def _tile(ref, i):
    return ref[SB * i : SB * (i + 1), :]


def chol_block(d_ref, e_ref):
    sub = _iota(0)
    lane = _iota(1)
    _set_identity(e_ref)
    for b in range(TILES):
        row_d = _tile(d_ref, b)
        row_e = _tile(e_ref, b)
        diag_cols = [_lane(row_d, SB * b + j) for j in range(SB)]
        scale = jnp.zeros((SB, NB), jnp.float32)
        inv, coef, rows_d, rows_e = [], [], [], []
        for j in range(SB):
            pivot = _sub(diag_cols[j], j)
            inv_j = 1.0 / pivot
            scale = jnp.where(sub == j, lax.rsqrt(pivot), scale)
            mult = jnp.where(sub > j, diag_cols[j] * inv_j, 0.0)
            coef_j = {}
            for jj in range(j + 1, SB):
                coef_j[jj] = _sub(diag_cols[jj], j)
                diag_cols[jj] = diag_cols[jj] - mult * coef_j[jj]
            rd = _sub(row_d, j)
            re = _sub(row_e, j)
            row_d = row_d - mult * rd
            row_e = row_e - mult * re
            inv.append(inv_j)
            coef.append(coef_j)
            rows_d.append(rd)
            rows_e.append(re)
        d_ref[SB * b : SB * (b + 1), :] = jnp.where(lane >= sub + SB * b, row_d * scale, 0.0)
        e_ref[SB * b : SB * (b + 1), :] = row_e * scale
        for i in range(b + 1, TILES):
            tile_d = _tile(d_ref, i)
            tile_e = _tile(e_ref, i)
            cols = [_lane(tile_d, SB * b + j) for j in range(SB)]
            for j in range(SB):
                mult = cols[j] * inv[j]
                for jj in range(j + 1, SB):
                    cols[jj] = cols[jj] - mult * coef[j][jj]
                tile_d = tile_d - mult * rows_d[j]
                tile_e = tile_e - mult * rows_e[j]
            d_ref[SB * i : SB * (i + 1), :] = tile_d
            e_ref[SB * i : SB * (i + 1), :] = tile_e


def lu_block(w_ref, r_ref, p_ref, e_ref, pi_ref, s_ref):
    sub = _iota(0)
    lane = _iota(1)
    _set_identity(e_ref)
    _set_identity(pi_ref)
    for b in range(TILES):
        row_w = _tile(w_ref, b)
        row_e = _tile(e_ref, b)
        row_r = _tile(r_ref, b)
        later = lane >= SB * (b + 1)
        diag_cols = [_lane(row_w, SB * b + j) for j in range(SB)]
        norm_cols = [_lane(row_r, SB * b + j) for j in range(SB)]
        signs = jnp.zeros((SB, NB), jnp.float32)
        p_tile = jnp.zeros((SB, NB), jnp.float32)
        l_tile = row_w
        inv, coef, rows_p, rows_e = [], [], [], []
        for j in range(SB):
            alpha = _sub(diag_cols[j], j)
            norm = _sub(norm_cols[j], j)
            sign = jnp.where(alpha >= 0, -1.0, 1.0)
            inv_j = 1.0 / (alpha - sign * norm)
            mult = jnp.where(sub > j, diag_cols[j] * inv_j, 0.0)
            coef_j = {}
            for jj in range(j + 1, SB):
                coef_j[jj] = _sub(diag_cols[jj], j) - sign * _sub(norm_cols[jj], j)
                diag_cols[jj] = diag_cols[jj] - mult * coef_j[jj]
            rp = _sub(row_w, j) - sign * _sub(row_r, j)
            re = _sub(row_e, j)
            row_w = row_w - mult * rp
            row_e = row_e - mult * re
            signs = jnp.where(sub == j, sign, signs)
            p_tile = jnp.where(sub == j, rp, p_tile)
            l_tile = jnp.where(lane == SB * b + j, mult, l_tile)
            inv.append(inv_j)
            coef.append(coef_j)
            rows_p.append(jnp.where(later, rp, 0.0))
            rows_e.append(re)
        s_ref[SB * b : SB * (b + 1), :] = signs
        e_ref[SB * b : SB * (b + 1), :] = row_e
        p_ref[SB * b : SB * (b + 1), :] = jnp.where(lane >= sub + SB * b, p_tile, 0.0)
        l_tile = jnp.where(lane == sub + SB * b, 1.0, l_tile)
        w_ref[SB * b : SB * (b + 1), :] = jnp.where(lane <= sub + SB * b, l_tile, 0.0)
        for i in range(b + 1, TILES):
            tile_w = _tile(w_ref, i)
            tile_e = _tile(e_ref, i)
            cols = [_lane(tile_w, SB * b + j) for j in range(SB)]
            for j in range(SB):
                mult = cols[j] * inv[j]
                for jj in range(j + 1, SB):
                    cols[jj] = cols[jj] - mult * coef[j][jj]
                tile_w = jnp.where(lane == SB * b + j, mult, tile_w - mult * rows_p[j])
                tile_e = tile_e - mult * rows_e[j]
            w_ref[SB * i : SB * (i + 1), :] = tile_w
            e_ref[SB * i : SB * (i + 1), :] = tile_e
        for i in range(b + 1):
            tile_pi = _tile(pi_ref, i)
            cols = [_lane(tile_pi, SB * b + j) for j in range(SB)]
            for j in range(SB):
                mult = cols[j] * inv[j]
                for jj in range(j + 1, SB):
                    cols[jj] = cols[jj] - mult * coef[j][jj]
                tile_pi = jnp.where(lane == SB * b + j, mult, tile_pi - mult * rows_p[j])
            pi_ref[SB * i : SB * (i + 1), :] = tile_pi


def window_starts(n, panels):
    width = n // panels
    return [min(width * g // NB * NB, n - 2 * NB) for g in range(panels)]


def slab_starts(n):
    starts, at = [], 0
    for top in range(0, n, SLAB):
        starts.append(at)
        at += n - top
    return starts, at


def gram_view(g_ref, n, lo, hi, first, last):
    starts, _ = slab_starts(n)
    slab = lo // SLAB
    base = starts[slab] - SLAB * slab
    return g_ref[lo - SLAB * slab : hi - SLAB * slab, base + first : base + last]


def factor_kernel(n, g_ref, at_ref, ft_ref, xt_ref, pit_ref, t_ref, tau_ref, flag_ref, a_ref, l_ref, p_ref, rh_ref, li_ref, pi_ref, d_ref, e_ref, w_ref, lie_ref, pd_ref, pie_ref, s_ref):
    blocks = n // NB

    def enter_step(i, carry):
        block = pl.ds(pl.multiple_of(NB * i, NB), NB)
        for ref in (xt_ref, pi_ref, l_ref, p_ref, rh_ref, li_ref):
            ref[block, :] = jnp.zeros((NB, n), jnp.float32)
        a_ref[block, :] = at_ref[:, block].T
        return carry

    lax.fori_loop(0, blocks, enter_step, 0)

    def block_step(g, carry):
        for i in range(blocks):
            lo = NB * i
            hi = lo + NB

            @pl.when(g == i)
            def _():
                d_new = gram_view(g_ref, n, lo, hi, lo, hi)
                w_new = a_ref[lo:hi, lo:hi]
                if i:
                    r_col = rh_ref[0:lo, lo:hi]
                    d_new = d_new - dot_tn(r_col, r_col)
                    w_new = w_new - dot_high(l_ref[lo:hi, 0:lo], p_ref[0:lo, lo:hi])
                d_ref[...] = d_new
                w_ref[...] = w_new

        chol_block(d_ref, e_ref)
        lu_block(w_ref, d_ref, pd_ref, lie_ref, pie_ref, s_ref)

        for i in range(blocks):
            lo = NB * i
            hi = lo + NB

            @pl.when(g == i)
            def _():
                signs = s_ref[...]
                r_gg = signs * d_ref[...]
                xt_gg = signs * e_ref[...]
                l_gg = w_ref[...]
                li_gg = lie_ref[...]
                p_gg = pd_ref[...]
                pi_gg = pie_ref[...]
                rh_ref[lo:hi, lo:hi] = r_gg
                xt_ref[lo:hi, lo:hi] = xt_gg
                l_ref[lo:hi, lo:hi] = l_gg
                li_ref[lo:hi, lo:hi] = li_gg
                p_ref[lo:hi, lo:hi] = p_gg
                pi_ref[lo:hi, lo:hi] = pi_gg
                if hi < n:
                    g_row = gram_view(g_ref, n, lo, hi, hi, n)
                    w_row = a_ref[lo:hi, hi:n]
                    w_col = a_ref[hi:n, lo:hi]
                    if i:
                        g_row = g_row - dot_tn(rh_ref[0:lo, lo:hi], rh_ref[0:lo, hi:n])
                        w_row = w_row - dot_high(l_ref[lo:hi, 0:lo], p_ref[0:lo, hi:n])
                        w_col = w_col - dot_high(l_ref[hi:n, 0:lo], p_ref[0:lo, lo:hi])
                    r_row = dot_high(xt_gg, g_row)
                    rh_ref[lo:hi, hi:n] = r_row
                    p_ref[lo:hi, hi:n] = dot_high(li_gg, w_row - r_row)
                    l_ref[hi:n, lo:hi] = dot_high(w_col, pi_gg)
                if i:
                    scaled = dot_high(p_ref[0:lo, lo:hi], pi_gg)
                    cut = NB * (i // 2)
                    for first, last in ((0, cut), (cut, lo)):
                        if first < last:
                            xt_ref[lo:hi, first:last] = -dot_high(xt_gg, dot_tn(rh_ref[first:lo, lo:hi], xt_ref[first:lo, first:last]))
                            pi_ref[first:last, lo:hi] = -dot_high(pi_ref[first:last, first:lo], scaled[first:lo])
                    prev = lo - NB
                    li_ref[lo:hi, prev:lo] = -dot_high(li_gg, dot_high(l_ref[lo:hi, prev:lo], li_ref[prev:lo, prev:lo]))

        return carry

    lax.fori_loop(0, blocks, block_step, 0)

    def leave_step(i, carry):
        block = pl.ds(pl.multiple_of(NB * i, NB), NB)
        rows = lax.broadcasted_iota(jnp.int32, (n, NB), 0)
        cols = lax.broadcasted_iota(jnp.int32, (n, NB), 1) + NB * i
        ft_ref[block, :] = jnp.where(rows <= cols, rh_ref[:, block], l_ref[:, block]).T
        pit_ref[block, :] = pi_ref[:, block].T
        return carry

    lax.fori_loop(0, blocks, leave_step, 0)
    windows = t_ref.shape[0]
    for w, start in enumerate(window_starts(n, windows)):
        one, two = slice(start, start + NB), slice(start + NB, start + 2 * NB)
        both = slice(start, start + 2 * NB)
        px_11 = dot_nt(p_ref[one, one], xt_ref[one, one])
        px_12 = dot_nt(p_ref[one, both], xt_ref[two, both])
        px_22 = dot_nt(p_ref[two, two], xt_ref[two, two])
        t_11 = -dot_nt(px_11, li_ref[one, one])
        t_12 = -dot_nt(px_11, li_ref[two, one]) - dot_nt(px_12, li_ref[two, two])
        t_22 = -dot_nt(px_22, li_ref[two, two])
        t_win = jnp.concatenate([jnp.concatenate([t_11, t_12], axis=1), jnp.concatenate([jnp.zeros_like(t_12), t_22], axis=1)], axis=0)
        width = t_ref.shape[1]
        off = width * w - start
        if off:
            t_win = pltpu.roll(t_win[off : off + width], 2 * NB - off, 1)
        t_fac = t_win[0:width, 0:width]
        t_ref[w] = t_fac
        t_diag = lax.broadcasted_iota(jnp.int32, (width, width), 0) == lax.broadcasted_iota(jnp.int32, (width, width), 1)
        tau_ref[w : w + 1, :] = jnp.sum(jnp.where(t_diag, t_fac, 0.0), axis=0, keepdims=True)
    total = jnp.zeros((1, 1), jnp.float32)
    on_diag = lax.broadcasted_iota(jnp.int32, (NB, NB), 0) == lax.broadcasted_iota(jnp.int32, (NB, NB), 1)
    for lo in range(0, n, NB):
        hi = lo + NB
        diag = jnp.sum(jnp.where(on_diag, gram_view(g_ref, n, lo, hi, lo, hi), 0.0), axis=0, keepdims=True)
        block = xt_ref[lo:n, lo:hi]
        total = total + jnp.sum(diag * jnp.sum(block * block, axis=0, keepdims=True), axis=1, keepdims=True)
    flag_ref[...] = jnp.broadcast_to(total, flag_ref.shape)


def factor_call(gram, top_t, panels):
    n = top_t.shape[0]
    square = jax.ShapeDtypeStruct((n, n), jnp.float32)
    vmem = pl.BlockSpec(memory_space=pltpu.VMEM)
    return pl.pallas_call(
        functools.partial(factor_kernel, n),
        out_shape=(
            square,
            square,
            square,
            jax.ShapeDtypeStruct((panels, n // panels, n // panels), jnp.float32),
            jax.ShapeDtypeStruct((panels, n // panels), jnp.float32),
            jax.ShapeDtypeStruct((SB, NB), jnp.float32),
        ),
        in_specs=[vmem, vmem],
        out_specs=(vmem,) * 6,
        scratch_shapes=[pltpu.VMEM((n, n), jnp.float32)] * 6 + [pltpu.VMEM((NB, NB), jnp.float32)] * 7,
        compiler_params=pltpu.CompilerParams(vmem_limit_bytes=30 * 1024 * 1024),
        cost_estimate=pl.CostEstimate(flops=20_000_000_000, bytes_accessed=20_000_000, transcendentals=0),
    )(gram, top_t)


def gram_kernel(at_ref, g_ref, top_ref, got_ref, got_s, top_s, full_s, part_s, red_s, r0_s, r1_s, r2_s, r3_s, half_send, half_recv, top_recv, top_xs, top_cs, top_ys, red_send, red_recv):
    panels_loc, width, rows_loc = at_ref.shape
    n = full_s.shape[0]
    half = rows_loc // 2
    chunk = full_s.shape[1]
    chunks = half // chunk
    col = lax.axis_index("col")
    row = lax.axis_index("row")
    core = row % 2
    to_y = {"col": 1 - col}
    to_core = {"row": row + 1 - 2 * core}
    to_x = {"row": (row + 2) % 4}
    barrier = pltpu.get_barrier_semaphore()
    for dev in (to_y, to_core, to_x):
        pl.semaphore_signal(barrier, inc=1, device_id=dev, device_id_type=MESH)
    pl.semaphore_wait(barrier, 3)

    def remote(src, dst, send, recv, dev):
        return pltpu.make_async_remote_copy(src_ref=src, dst_ref=dst, send_sem=send, recv_sem=recv, device_id=dev, device_id_type=MESH)

    halves = []
    for k in range(chunks):
        lanes = pl.ds(pl.multiple_of(half * (1 - col) + chunk * k, NB), chunk)
        copy = remote(at_ref.at[:, :, lanes], got_s.at[:, :, chunk * k : chunk * (k + 1)], half_send.at[k], half_recv.at[k], to_y)
        copy.start()
        halves.append(copy)

    top_chunk = n // chunks

    def top_copies(src, which, send, dev):
        pieces = [slice(top_chunk * k, top_chunk * (k + 1)) for k in range(chunks)]
        return [remote(src.at[:, :, p], top_s.at[which, :, :, p], send.at[k], top_recv.at[which, k], dev) for k, p in enumerate(pieces)]

    own_top = at_ref.at[:, :, 0:n]
    is_first = (row == 0) & (col == 0)
    is_second = (row == 0) & (col == 1)

    @pl.when(row == 0)
    def _():
        for to_one, to_two in zip(top_copies(own_top, col, top_xs.at[0], to_x), top_copies(own_top, col, top_cs.at[0], to_core)):
            to_one.start()
            to_two.start()

    @pl.when(is_first)
    def _():
        for copy in top_copies(own_top, 0, top_ys, to_y):
            copy.start()

    starts, _ = slab_starts(n)
    part_s[...] = jnp.zeros_like(part_s)

    def gram_step(k, carry):
        here = pl.ds(pl.multiple_of(chunk * k, NB), chunk)
        theirs = pl.ds(pl.multiple_of(half * (1 - col) + chunk * k, NB), chunk)
        remote(at_ref.at[:, :, theirs], got_s.at[:, :, here], half_send.at[k], half_recv.at[k], to_y).wait_recv()

        @pl.when(is_first)
        def _():
            for send, dev in ((top_xs, to_x), (top_cs, to_core)):
                remote(got_s.at[:, :, here], top_s.at[1, :, :, here], send.at[1, k], top_recv.at[1, k], dev).start()

        mine = pl.ds(pl.multiple_of(half * col + chunk * k, NB), chunk)
        for s in range(panels_loc):
            full_s[pl.ds(pl.multiple_of(width * (2 * s + col), SB), width), :] = at_ref[s, :, mine]
            full_s[pl.ds(pl.multiple_of(width * (2 * s + 1 - col), SB), width), :] = got_s[s, :, here]
        for i, at in enumerate(starts):
            lo = SLAB * i
            part_s[:, at : at + n - lo] += dot_nt(full_s[lo : lo + SLAB, :], full_s[lo:n, :])
        return carry

    lax.fori_loop(0, chunks, gram_step, 0)

    per_core = SLAB // 2
    quarter = per_core // 2
    mine = pl.ds(pl.multiple_of(per_core * core, SB), per_core)
    other = pl.ds(pl.multiple_of(per_core * (1 - core), SB), per_core)
    pair = remote(part_s.at[other, :], r0_s, red_send.at[0], red_recv.at[0], to_core)
    pair.start()
    pair.wait_recv()
    red_s[0] = part_s[mine, :] + r0_s[...]
    first = [
        remote(red_s.at[0, 0:quarter, :], r1_s.at[0], red_send.at[1], red_recv.at[1], to_x),
        remote(red_s.at[0, quarter:per_core, :], r1_s.at[1], red_send.at[2], red_recv.at[2], to_y),
    ]
    for copy in first:
        copy.start()

    @pl.when(is_second)
    def _():
        came = top_copies(own_top, 0, top_ys, to_y)
        for k, copy in enumerate(came):
            copy.wait_recv()
            top_copies(top_s.at[0], 0, top_xs.at[1], to_x)[k].start()
            top_copies(top_s.at[0], 0, top_cs.at[1], to_core)[k].start()

    for k, copy in enumerate(first):
        copy.wait_recv()
        red_s[1, quarter * k : quarter * (k + 1), :] = red_s[0, quarter * k : quarter * (k + 1), :] + r1_s[k]
    second = [
        remote(red_s.at[1, 0:quarter, :], r2_s.at[0], red_send.at[3], red_recv.at[3], to_y),
        remote(red_s.at[1, quarter:per_core, :], r2_s.at[1], red_send.at[4], red_recv.at[4], to_x),
    ]
    for copy in second:
        copy.start()

    for k, copy in enumerate(second):
        copy.wait_recv()
        red_s[2, quarter * k : quarter * (k + 1), :] = red_s[1, quarter * k : quarter * (k + 1), :] + r2_s[k]
    last = remote(red_s.at[2], r3_s, red_send.at[5], red_recv.at[5], to_core)
    last.start()
    g_ref[mine, :] = red_s[2]

    @pl.when(row == 2)
    def _():
        for step in range(2):
            which = col if step == 0 else 1 - col
            came = top_copies(own_top, which, top_xs.at[step], to_x)
            sent = top_copies(top_s.at[which], which, top_cs.at[step], to_core)
            for k in range(chunks):
                came[k].wait_recv()
                sent[k].start()

    last.wait_recv()
    g_ref[other, :] = r3_s[...]

    @pl.when(core == 1)
    def _():
        for step in range(2):
            for copy in top_copies(own_top, col if step == 0 else 1 - col, top_cs.at[step], to_core):
                copy.wait_recv()


    def leave_step(k, carry):
        lanes = pl.ds(pl.multiple_of(NB * k, NB), NB)
        got_ref[:, :, lanes] = got_s[:, :, lanes]

        @pl.when(row != 0)
        def _():
            for s in range(panels_loc):
                for c in range(2):
                    top_ref[2 * s + c, :, lanes] = top_s[c, s, :, lanes]

        @pl.when(row == 0)
        def _():
            for s in range(panels_loc):
                top_ref[2 * s + col, :, lanes] = at_ref[s, :, lanes]

        @pl.when(is_first)
        def _():
            for s in range(panels_loc):
                top_ref[2 * s + 1, :, lanes] = got_s[s, :, lanes]

        @pl.when(is_second)
        def _():
            for s in range(panels_loc):
                top_ref[2 * s, :, lanes] = top_s[0, s, :, lanes]

        return carry

    lax.fori_loop(0, n // NB, leave_step, 0)

    for copy in halves + [pair] + first + second + [last]:
        copy.wait_send()

    @pl.when(is_first)
    def _():
        for copy in top_copies(own_top, 0, top_ys, to_y):
            copy.wait_send()

    @pl.when(row == 0)
    def _():
        for step in range(2):
            for copy in top_copies(own_top, col, top_xs.at[step], to_x):
                copy.wait_send()

    @pl.when(core == 0)
    def _():
        for step in range(2):
            for copy in top_copies(own_top, col, top_cs.at[step], to_core):
                copy.wait_send()


def gram_call(a_t, n):
    panels_loc, width, rows_loc = a_t.shape
    half = rows_loc // 2
    _, packed = slab_starts(n)
    vmem = pl.BlockSpec(memory_space=pltpu.VMEM)
    per_core = SLAB // 2
    f32 = lambda *shape: pltpu.VMEM(shape, jnp.float32)
    dma = pltpu.SemaphoreType.DMA
    chunks = 6
    return pl.pallas_call(
        gram_kernel,
        out_shape=(
            jax.ShapeDtypeStruct((SLAB, packed), jnp.float32),
            jax.ShapeDtypeStruct((2 * panels_loc, width, n), jnp.float32),
            jax.ShapeDtypeStruct((panels_loc, width, half), jnp.float32),
        ),
        in_specs=[vmem],
        out_specs=(vmem,) * 3,
        scratch_shapes=[
            f32(panels_loc, width, half),
            f32(2, panels_loc, width, n),
            f32(n, half // chunks),
            f32(SLAB, packed),
            f32(3, per_core, packed),
            f32(per_core, packed),
            f32(2, per_core // 2, packed),
            f32(2, per_core // 2, packed),
            f32(per_core, packed),
            dma((chunks,)),
            dma((chunks,)),
            dma((2, chunks)),
            dma((2, chunks)),
            dma((2, chunks)),
            dma((chunks,)),
            dma((6,)),
            dma((6,)),
        ],
        compiler_params=pltpu.CompilerParams(vmem_limit_bytes=22 * 1024 * 1024, collective_id=0, has_side_effects=True),
        cost_estimate=pl.CostEstimate(flops=10_000_000_000, bytes_accessed=10_000_000, transcendentals=0),
    )(a_t)


def apply_kernel(at_ref, got_ref, far_ref, xt_ref, pit_ref, ft_ref, q_ref, v_ref, full_s, own_s):
    panels_loc, width, chunk = at_ref.shape
    n = xt_ref.shape[0]
    step = pl.program_id(0)
    col = lax.axis_index("col")
    row = lax.axis_index("row")
    steps_half = pl.num_programs(0) // 2
    near = (step // steps_half) == col

    for s in range(panels_loc):
        full_s[pl.ds(pl.multiple_of(width * (2 * s + col), SB), width), :] = at_ref[s]
        full_s[pl.ds(pl.multiple_of(width * (2 * s + 1 - col), SB), width), :] = jnp.where(near, got_ref[s], far_ref[s])
    for lo in range(0, n, SLAB):
        hi = lo + SLAB
        q_ref[:, lo:hi] = lax.dot_general(full_s[0:hi, :], xt_ref[lo:hi, 0:hi], (((0,), (1,)), ((), ())), precision=HIGHEST, preferred_element_type=jnp.float32)
    is_top = (row == 0) & (step < n // chunk)

    @pl.when(jnp.logical_not(is_top))
    def _():
        for s in range(panels_loc):
            depth = width * 2 * (s + 1)
            rows = pl.ds(pl.multiple_of(width * (2 * s + col), SB), width)
            v_ref[s] = dot_high(pit_ref[rows, 0:depth], full_s[0:depth, :])

    @pl.when(is_top)
    def _():
        lanes = pl.ds(pl.multiple_of(jnp.minimum(step, n // chunk - 1) * chunk, NB), chunk)
        for s in range(panels_loc):
            rows = pl.ds(pl.multiple_of(width * (2 * s + col), SB), width)
            v_ref[s] = ft_ref[rows, lanes]


def apply_call(a_t, got, far, x_t, pi_t, f_t):
    panels_loc, width, rows_loc = a_t.shape
    n = x_t.shape[0]
    chunk = 256
    steps = rows_loc // chunk
    half_steps = steps // 2
    part = lambda index: pl.BlockSpec((panels_loc, width, chunk), index)
    whole = pl.BlockSpec(memory_space=pltpu.VMEM)
    return pl.pallas_call(
        apply_kernel,
        grid=(steps,),
        out_shape=(jax.ShapeDtypeStruct((rows_loc, n), jnp.float32), jax.ShapeDtypeStruct((panels_loc, width, rows_loc), jnp.float32)),
        in_specs=[part(lambda i: (0, 0, i)), part(lambda i: (0, 0, i % half_steps)), part(lambda i: (0, 0, i % half_steps)), whole, whole, whole],
        out_specs=(pl.BlockSpec((chunk, n), lambda i: (i, 0)), part(lambda i: (0, 0, i))),
        scratch_shapes=[pltpu.VMEM((n, chunk), jnp.float32), pltpu.VMEM((SB, NB), jnp.float32)],
        compiler_params=pltpu.CompilerParams(vmem_limit_bytes=24 * 1024 * 1024),
        cost_estimate=pl.CostEstimate(flops=5_000_000_000, bytes_accessed=20_000_000, transcendentals=0),
    )(a_t, got, far, x_t, pi_t, f_t)


def solution(mesh):
    proc_cols = mesh.shape["col"]

    def local_program(a_loc):
        rows_loc, panels_loc, panel_width = a_loc.shape
        num_panels = panels_loc * proc_cols
        n = num_panels * panel_width
        col_idx = lax.axis_index("col")
        half = rows_loc // proc_cols
        a_t = a_loc.transpose(1, 2, 0)
        gram, top_t, got = gram_call(a_t, n)
        own_half = lax.dynamic_slice_in_dim(a_t, col_idx * half, half, axis=2)
        own_half, gram, top_t, got = lax.optimization_barrier((own_half, gram, top_t, got))
        far = lax.ppermute(own_half, "col", [(0, 1), (1, 0)])
        f_t, x_t, pi_t, t_facs, taus, flag = factor_call(gram, top_t.reshape(n, n), num_panels)
        well = flag[0, 0] < 2.0 * n

        def gram_path(_):
            q_rows, vecs = apply_call(a_t, got, far, x_t, pi_t, f_t)
            return vecs.transpose(2, 0, 1), taus, t_facs, q_rows

        return lax.cond(well, gram_path, lambda _: columnwise_program(a_loc.transpose(1, 2, 0), proc_cols, mesh.shape["row"]), 0)

    spec_rows = P(("part", "row"), "col", None)
    out_specs = (spec_rows, P("part", None), P("part", None, None), P(("part", "row"), None))
    return jax.shard_map(local_program, mesh=mesh, in_specs=(spec_rows,), out_specs=out_specs, check_vma=False)
```
